32 devices in a mesh: frag: 2 (over x), grid: 16 (over z, y, core).
Axes of the slice: x: 2, y: 2, z: 4, core: 2. Of those that a mesh axis runs over, the one named last changes fastest.
Arguments:
- psi: float32 [16384, 640], P(('frag', 'grid')), parts along dimension 0
- order: int32 [10], P('frag'), parts along dimension 0, may hold values from 0 to 4, each once
Outputs:
- orthonormal: float32 [16384, 640], P(('frag', 'grid')), parts along dimension 0
The draws below stay inside these ranges and needn't reach their ends.
There are 2 independent parts, one for each index of `frag`. The reference program is written for one: setup_inputs(seed, part) draws one part's arguments, and reference() takes and returns one part's arrays. A program takes and returns all parts, laid end to end along the dimension named above; each array names one. Nothing has to cross between parts.
All inputs are finite; a program needn't handle non-finite values.
Results may differ from the reference program's by a relative error of at most 0.00012.
Values sent between devices are 32-bit elements; how exact they have to be, the bound alone decides.
A program may use at most 64 MiB of HBM per device.

```python
import jax
import jax.numpy as jnp
from jax import lax

BLOCK = 128
NBLK = 5
BANDS = 640
POINTS = 8192


def draw_psi(key, part):
    own = jax.random.normal(jax.random.fold_in(key, 11), (POINTS, BANDS), jnp.float32)
    shared = jax.random.normal(jax.random.fold_in(key, 12), (POINTS, BLOCK), jnp.float32)
    mixed = own + 0.8 * jnp.tile(shared, (1, NBLK))
    return mixed.astype(jnp.float32)


def setup_inputs(seed: int = 0, part: int = 0) -> dict:
    streams_of = jax.random.split(jax.random.key(seed), 3)
    part_splits = jax.random.split(jax.random.fold_in(streams_of[2], part), 3)
    psi = draw_psi(jax.random.fold_in(jax.random.fold_in(streams_of[2], part), 71), part)
    order = jax.random.permutation(part_splits[1], NBLK).astype(jnp.int32)
    return {"psi": psi, "order": order}


def contract(left, right):
    return lax.dot_general(left.astype(jnp.float32), right.astype(jnp.float32), (((0,), (0,)), ((), ())), precision=lax.Precision.HIGHEST, preferred_element_type=jnp.float32)

def matmul(left, right):
    return jnp.dot(left.astype(jnp.float32), right.astype(jnp.float32), precision=lax.Precision.HIGHEST, preferred_element_type=jnp.float32)

def reference(psi, order):
    scale = jnp.float32(1.0 / POINTS)
    result = jnp.zeros_like(psi)
    done = []
    for step in range(NBLK):
        start = (order[step] * BLOCK).astype(jnp.int32)
        block = lax.dynamic_slice_in_dim(psi, start, BLOCK, 1)
        if step > 0:
            prev = jnp.concatenate(done, axis=1)
            coeff = contract(prev, block) * scale
            block = block - matmul(prev, coeff)
        gram = contract(block, block) * scale
        lower = jnp.linalg.cholesky(gram)
        inverse = lax.linalg.triangular_solve(lower, jnp.eye(BLOCK, dtype=gram.dtype), left_side=True, lower=True)
        basis = matmul(block, inverse.T)
        done.append(basis)
        result = lax.dynamic_update_slice(result, basis, (jnp.int32(0), start))
    return result
```

```python
import functools

import jax
import jax.numpy as jnp
from jax import lax
from jax.experimental import pallas as pl
from jax.experimental.pallas import tpu as pltpu
from jax.sharding import PartitionSpec as P

BLOCK = 128
PANEL = 16
TILE = 8
HIGHEST = lax.Precision.HIGHEST


def dot(left, right, dims):
    return lax.dot_general(
        left, right, (dims, ((), ())), precision=HIGHEST, preferred_element_type=jnp.float32
    )


CUTS = ((), (1,), (1,), (1, 2), (1, 2))
EVENTS = (
    (1, 2, 0, 3, 4, 1, 0),
    (2, 3), (4,), (1,), (2,), (3,), (1, 4), (2,), (3,),
    (4,), (3,), (4,), (3,), (4,), (4,),
)


def thirds(value):
    high = value.astype(jnp.bfloat16)
    value = value - high.astype(jnp.float32)
    middle = value.astype(jnp.bfloat16)
    return high, middle, (value - middle.astype(jnp.float32)).astype(jnp.bfloat16)


def factor_block(gram, result):
    tiles = PANEL // TILE
    row = lax.broadcasted_iota(jnp.int32, (TILE, BLOCK), 0)
    lane = lax.broadcasted_iota(jnp.int32, (TILE, BLOCK), 1)
    rest, done = gram, []
    for start in range(0, BLOCK, PANEL):
        panel = [rest[r * TILE : (r + 1) * TILE, :] for r in range(tiles)]
        columns = [
            [jnp.broadcast_to(panel[r][:, start + j : start + j + 1], (TILE, BLOCK)) for r in range(tiles)]
            for j in range(PANEL)
        ]
        inside = (lane >= start) & (lane < start + PANEL)
        panel = [
            jnp.where(inside, jnp.where(lane == row + (start + r * TILE), 1.0, 0.0), panel[r])
            for r in range(tiles)
        ]
        pivots = [jnp.ones((TILE, BLOCK), jnp.float32)] * tiles
        for j in range(PANEL):
            own, sub = divmod(j, TILE)
            pivot = jnp.broadcast_to(columns[j][own][sub : sub + 1, :], (TILE, BLOCK))
            pivots[own] = jnp.where(row == sub, pivot, pivots[own])
            if j == PANEL - 1:
                break
            inverse = 1.0 / pivot
            factors = {}
            for r in range(own, tiles):
                value = columns[j][r] * inverse
                factors[r] = jnp.where(row > sub, value, 0.0) if r == own else value
            targets = columns[j + 1 :] + [panel]
            for target in targets:
                top = jnp.broadcast_to(target[own][sub : sub + 1, :], (TILE, BLOCK))
                for r in range(own, tiles):
                    target[r] = target[r] - factors[r] * top
        norm = jnp.concatenate([panel[r] * lax.rsqrt(pivots[r]) for r in range(tiles)], axis=0)
        wide = lax.broadcasted_iota(jnp.int32, (PANEL, BLOCK), 1)
        done.append(jnp.where(wide < start + PANEL, norm, 0.0))
        yield
        left = BLOCK - start - PANEL
        if left:
            high, middle, low = thirds(norm)
            left_parts = jnp.concatenate([low, high, middle, middle, high, high], axis=0)
            right_parts = jnp.concatenate([high, low, middle, high, middle, high], axis=0)
            turned = left_parts.T
            cuts = [start + PANEL, start + 2 * PANEL, BLOCK]
            update = jnp.concatenate(
                [
                    jnp.dot(turned[a:b, :], right_parts, preferred_element_type=jnp.float32)
                    for a, b in zip(cuts, cuts[1:])
                    if a < b
                ],
                axis=0,
            )
            wide = lax.broadcasted_iota(jnp.int32, (left, BLOCK), 1)
            inside = (wide >= start) & (wide < start + PANEL)
            rest = jnp.where(inside, 0.0, rest[PANEL:, :]) - update
    result.append(jnp.concatenate(done, axis=0))


class Exchange:
    def __init__(self, bits, refs):
        self.me = lax.axis_index("grid")
        self.digit = [(self.me // 2**k) % 2 for k in range(bits)]
        self.part, self.acc, self.recv, self.full, self.send_sem, self.recv_sem = refs
        self.used = 0
        self.sent = []

    def toward(self, low, delta):
        shift = 0
        for k in range(delta.bit_length()):
            if (delta >> k) & 1:
                shift = shift + (1 - 2 * self.digit[low + k]) * 2**k
        return shift

    def send(self, src, dst, low, delta):
        copy = pltpu.make_async_remote_copy(
            src_ref=src,
            dst_ref=dst,
            send_sem=self.send_sem.at[self.used],
            recv_sem=self.recv_sem.at[self.used],
            device_id={"grid": self.me + self.toward(low, delta) * 2**low},
            device_id_type=pl.DeviceIdType.MESH,
        )
        copy.start()
        self.used += 1
        self.sent.append(copy)
        return copy

    def steps(self, at, rows, stages):
        offset, size, base = at, rows, at
        last = len(stages) - 1
        for i, (low, high) in enumerate(stages):
            group = 2 ** (high - low)
            own = (self.me // 2**low) % group
            sub = size // group
            source = self.part if i == 0 else self.acc
            copies = []
            for delta in range(1, group):
                give = pl.multiple_of(offset + (own + self.toward(low, delta)) * sub, TILE)
                slot = base + (delta - 1) * sub
                copies.append(
                    self.send(source.at[pl.ds(give, sub)], self.recv.at[pl.ds(slot, sub)], low, delta)
                )
            yield
            keep = pl.multiple_of(offset + own * sub, TILE)
            total = source[pl.ds(keep, sub), :]
            for delta, copy in enumerate(copies):
                copy.wait_recv()
                total = total + self.recv[base + delta * sub : base + (delta + 1) * sub, :]
            target = self.full if i == last else self.acc
            target[pl.ds(keep, sub), :] = total
            offset, size, base = keep, sub, base + (group - 1) * sub
        for low, high in reversed(stages):
            group = 2 ** (high - low)
            own = (self.me // 2**low) % group
            here = self.full.at[pl.ds(pl.multiple_of(offset, TILE), size)]
            copies = [self.send(here, here, low, delta) for delta in range(1, group)]
            yield
            for copy in copies:
                copy.wait_recv()
            offset, size = offset - own * size, size * group


def stages_of(bits, column):
    cuts = sorted({0, *CUTS[min(column, len(CUTS) - 1)], bits})
    cuts = [c for c in cuts if c <= bits]
    return list(zip(cuts, cuts[1:]))


def copies_of(stages):
    return 2 * sum(2 ** (high - low) - 1 for low, high in stages)


def fused_kernel(
    bits, scale, ats, order_ref, psi_ref, q,
    x, part, acc, recv, full, work, norms, inverses, send_sem, recv_sem,
):
    count = order_ref.shape[0]
    me = lax.axis_index("grid")

    def span(i):
        return slice(i * BLOCK, (i + 1) * BLOCK)

    barrier = pltpu.get_barrier_semaphore()
    exchange = Exchange(bits, (part, acc, recv, full, send_sem, recv_sem))
    for delta in range(1, 2**bits):
        pl.semaphore_signal(
            barrier,
            inc=1,
            device_id={"grid": me + exchange.toward(0, delta)},
            device_id_type=pl.DeviceIdType.MESH,
        )

    for s in range(count):
        which = jnp.full((psi_ref.shape[0], BLOCK), order_ref[s], jnp.int32)
        block = psi_ref[:, span(0)]
        for b in range(1, count):
            block = jnp.where(which == b, psi_ref[:, span(b)], block)
        x[:, span(s)] = block

    pieces = []
    for t in range(count):
        at, rows = ats[t], (t + 1) * BLOCK
        part[at : at + rows, :] = dot(x[:, :rows], x[:, span(t)], ((0,), (0,))) * scale
        if at + rows < ats[t + 1]:
            part[at + rows : ats[t + 1], :] = jnp.zeros((ats[t + 1] - at - rows, BLOCK), jnp.float32)
        if t == 0:
            pl.semaphore_wait(barrier, 2**bits - 1)
        pieces.append(exchange.steps(at, ats[t + 1] - at, stages_of(bits, t)))
        next(pieces[t])

    alive = [True] * count

    def advance(t):
        if alive[t] and next(pieces[t], None) is None and pieces[t].gi_frame is None:
            alive[t] = False
            for r in range(t + 1):
                work[span(r), span(t)] = full[ats[t] + r * BLOCK : ats[t] + (r + 1) * BLOCK, :]

    def apply(s, t):
        norm = dot(inverses[span(s), :], work[span(s), span(t)], ((1,), (0,)))
        norms[span(s), span(t)] = norm
        left = norms[span(s), (s + 1) * BLOCK : (t + 1) * BLOCK]
        work[(s + 1) * BLOCK : (t + 1) * BLOCK, span(t)] -= dot(left, norm, ((0,), (0,)))

    def project(s, t):
        x[:, span(t)] -= dot(q[:, span(s)], norms[span(s), span(t)], ((1,), (0,)))

    todo = []
    events = list(EVENTS)
    for t in events.pop(0):
        advance(t)
    while alive[0]:
        advance(0)
    for s in range(count):
        while alive[s]:
            advance(s)
        for u in range(s):
            if ("a", u, s) in todo:
                todo.remove(("a", u, s))
                apply(u, s)
        result = []
        for _ in factor_block(work[span(s), span(s)], result):
            for t in events.pop(0) if events else ():
                if t < count:
                    advance(t)
            for item in [i for i in todo if i[0] == "a" and not alive[i[2]]][:1]:
                todo.remove(item)
                apply(item[1], item[2])
            else:
                for item in [i for i in todo if i[0] == "x" and ("a", i[1], i[2]) not in todo][:1]:
                    todo.remove(item)
                    project(item[1], item[2])
        inverses[span(s), :] = result[0]
        todo += [("a", s, t) for t in range(s + 1, count)]
        for u in range(s):
            if ("x", u, s) in todo:
                todo.remove(("x", u, s))
                project(u, s)
        q[:, span(s)] = dot(x[:, span(s)], inverses[span(s), :], ((1,), (1,)))
        todo += [("x", s, t) for t in range(s + 1, count)]

    for copy in exchange.sent:
        copy.wait_send()


def orthonormalize(devices, psi, order):
    count = order.shape[0]
    points, bands = psi.shape
    bits = devices.bit_length() - 1
    unit, ats = devices * TILE, [0]
    for t in range(count):
        ats.append(ats[-1] + -(-(t + 1) * BLOCK // unit) * unit)
    copies = sum(copies_of(stages_of(bits, t)) for t in range(count))
    scale = float(1.0 / (points * devices))
    vmem = pl.BlockSpec(memory_space=pltpu.VMEM)
    buffer = pltpu.VMEM((ats[-1], BLOCK), jnp.float32)
    square = pltpu.VMEM((bands, bands), jnp.float32)
    tall = pltpu.VMEM((points, bands), jnp.float32)
    semaphores = pltpu.SemaphoreType.DMA((copies,))
    return pl.pallas_call(
        functools.partial(fused_kernel, bits, scale, ats),
        out_shape=jax.ShapeDtypeStruct((points, bands), jnp.float32),
        in_specs=[pl.BlockSpec(memory_space=pltpu.SMEM), vmem],
        out_specs=vmem,
        scratch_shapes=[
            tall, buffer, buffer, buffer, buffer, square, square,
            pltpu.VMEM((bands, BLOCK), jnp.float32), semaphores, semaphores,
        ],
        compiler_params=pltpu.CompilerParams(collective_id=0, has_side_effects=True),
    )(order, psi)


def place_kernel(order_ref, q_ref, out_ref, held, in_sem, out_sem):
    count = order_ref.shape[0]
    loads, stores = [], []
    for s in range(count):
        columns = slice(s * BLOCK, (s + 1) * BLOCK)
        loads.append(pltpu.make_async_copy(q_ref.at[:, columns], held.at[s], in_sem.at[s]))
        loads[s].start()
    for s in range(count):
        home = pl.ds(pl.multiple_of(order_ref[s] * BLOCK, BLOCK), BLOCK)
        stores.append(pltpu.make_async_copy(held.at[s], out_ref.at[:, home], out_sem.at[s]))
        loads[s].wait()
        stores[s].start()
    for s in range(count):
        stores[s].wait()


def place(q, order):
    count = order.shape[0]
    rows, bands = q.shape
    anywhere = pl.BlockSpec(memory_space=pl.ANY)
    semaphores = pltpu.SemaphoreType.DMA((count,))
    return pl.pallas_call(
        place_kernel,
        out_shape=jax.ShapeDtypeStruct((rows, bands), jnp.float32),
        in_specs=[pl.BlockSpec(memory_space=pltpu.SMEM), anywhere],
        out_specs=anywhere,
        scratch_shapes=[pltpu.VMEM((count, rows, BLOCK), jnp.float32), semaphores, semaphores],
    )(order, q)


def solution(mesh):
    devices = mesh.shape["grid"]

    def local(psi, order):
        return place(orthonormalize(devices, psi, order), order)

    in_specs = (P(("frag", "grid"), None), P("frag"))
    out_specs = P(("frag", "grid"), None)
    return jax.shard_map(local, mesh=mesh, in_specs=in_specs, out_specs=out_specs, check_vma=False)
```
